32 devices in a mesh: sp: 4 (over z), tp: 8 (over y, x, core).
Axes of the slice: x: 2, y: 2, z: 4, core: 2. Of those that a mesh axis runs over, the one named last changes fastest.
Arguments:
- tokens: bfloat16 [8192, 2048], P(('sp', 'tp')), may hold values from -3 to 3
- queries: bfloat16 [8192, 2048], P(('sp', 'tp')), may hold values from -140 to 140
- keys: bfloat16 [8192, 1024], P(('sp', 'tp')), may hold values from -6 to 6
- values: bfloat16 [8192, 1024], P(('sp', 'tp')), may hold values from -6 to 6
- out_weight: bfloat16 [2048, 2048], P('sp', 'tp'), may hold values from -0.25 to 0.25
- norm_gain: bfloat16 [2048], replicated, may hold values from 0.099609375 to 1.8984375
- gate_weight: bfloat16 [2048, 7168], P('sp', 'tp'), may hold values from -0.125 to 0.125
- up_weight: bfloat16 [2048, 7168], P('sp', 'tp'), may hold values from -0.125 to 0.125
- down_weight: bfloat16 [7168, 2048], P('tp', 'sp'), may hold values from -0.125 to 0.125
Outputs:
- attended: bfloat16 [8192, 2048], P(('sp', 'tp'))
- layer_out: bfloat16 [8192, 2048], P(('sp', 'tp'))
The draws below stay inside these ranges and needn't reach their ends.
All inputs are finite; a program needn't handle non-finite values.
Results may differ from the reference program's by a relative error of at most 0.023.
Values may be sent and summed in bfloat16 or wider, within the bound.
A program may use at most 256 MiB of HBM per device.

```python
import jax
import jax.numpy as jnp
from jax import lax

D = 2048
FF = 7168
HEADS = 16
KV_HEADS = 8
HEAD_DIM = 128
TOK_DEV = 2048
SEQ = 8192
N_TP = 8


def shared_keys(key):
    sub_key = jax.random.fold_in(key, 5)
    base_draw = jnp.clip(jax.random.normal(sub_key, (SEQ, KV_HEADS * HEAD_DIM), jnp.float32), -5.0, 5.0)
    return base_draw


def draw_keys(key, part):
    return shared_keys(key).astype(jnp.bfloat16)


def draw_queries(key, part):
    sub_key = jax.random.fold_in(key, 9)
    base_draw = jnp.clip(2.5 * jax.random.normal(sub_key, (SEQ, HEADS * HEAD_DIM), jnp.float32), -15.0, 15.0)
    return base_draw.astype(jnp.bfloat16)


def level_of(own_key, dims, cuts, smallest, high):
    level = 1.0
    for position, shards_of in cuts:
        steps = jax.random.uniform(jax.random.fold_in(jax.random.fold_in(own_key, 6), position), (shards_of,), jnp.float32, smallest / len(cuts), high / len(cuts))
        level = level * jnp.repeat(jnp.exp(steps), dims[position] // shards_of).reshape((-1,) + (1,) * (len(dims) - 1 - position))
    return level


def scatter_about(stream_key, dims, width, most, shards=(), held_as=jnp.bfloat16):
    result = width * jax.random.normal(stream_key, dims, jnp.float32)
    if shards:
        result = result * level_of(stream_key, dims, shards, -0.22, 0.18)
    return jnp.clip(result, -most, most).astype(held_as)


def setup_inputs(seed: int = 0) -> dict:
    splits = jax.random.split(jax.random.key(seed), 10)
    return {
        "tokens": scatter_about(splits[0], (SEQ, D), 0.5, 3.0, ((0, 32),)),
        "queries": draw_queries(jax.random.fold_in(splits[9], 71), 0),
        "keys": draw_keys(jax.random.fold_in(splits[9], 71), 0),
        "values": scatter_about(splits[3], (SEQ, KV_HEADS * HEAD_DIM), 1.0, 6.0, ((0, 32),)),
        "out_weight": scatter_about(splits[4], (HEADS * HEAD_DIM, D), (HEADS * HEAD_DIM // 4) ** -0.5, 0.25, ((0, 4), (1, 8))),
        "norm_gain": jnp.clip(1.0 + 0.18 * jax.random.normal(splits[5], (D,), jnp.float32), 0.099609375, 1.8984375).astype(jnp.bfloat16),
        "gate_weight": scatter_about(splits[6], (D, FF), D ** -0.5, 0.125, ((0, 4), (1, 8))),
        "up_weight": scatter_about(splits[7], (D, FF), D ** -0.5, 0.125, ((0, 4), (1, 8))),
        "down_weight": scatter_about(splits[8], (FF, D), (FF // 4) ** -0.5, 0.125, ((0, 8), (1, 4))),
    }


def one_group(inputs):
    q_head, k_head, v_head = inputs
    seq_len = k_head.shape[0]
    group_size = q_head.shape[1]
    k_wide = k_head.astype(jnp.float32)
    v_wide = v_head.astype(jnp.float32)
    block_count = seq_len // TOK_DEV
    q_blocks = q_head.reshape(block_count, TOK_DEV, group_size, HEAD_DIM)
    starts = jnp.arange(block_count, dtype=jnp.int32) * TOK_DEV
    key_pos = jnp.arange(seq_len, dtype=jnp.int32)

    def one_block(pair):
        q_block, start = pair
        scores = jnp.einsum('qgd,kd->gqk', q_block.astype(jnp.float32), k_wide) * HEAD_DIM ** (-0.5)
        query_pos = start + jnp.arange(TOK_DEV, dtype=jnp.int32)
        causal = key_pos[None, :] <= query_pos[:, None]
        scores = jnp.where(causal[None, :, :], scores, -1e+30)
        row_peak = lax.optimization_barrier(jnp.max(scores, axis=-1, keepdims=True))
        exp_terms = jnp.exp(scores - row_peak)
        probs = (exp_terms / lax.optimization_barrier(jnp.sum(exp_terms, axis=-1, keepdims=True))).astype(jnp.bfloat16)
        mixed_out = jnp.einsum('gqk,kd->qgd', probs.astype(jnp.float32), v_wide)
        return mixed_out.astype(jnp.bfloat16)
    blocks_out = lax.map(one_block, (q_blocks, starts))
    return blocks_out.reshape(seq_len, group_size, HEAD_DIM)

def reference(tokens, queries, keys, values, out_weight, norm_gain, gate_weight, up_weight, down_weight):
    seq_len = tokens.shape[0]
    group_size = HEADS // KV_HEADS
    q_stack = jnp.transpose(queries.reshape(seq_len, KV_HEADS, group_size, HEAD_DIM), (1, 0, 2, 3))
    k_stack = jnp.transpose(keys.reshape(seq_len, KV_HEADS, HEAD_DIM), (1, 0, 2))
    v_stack = jnp.transpose(values.reshape(seq_len, KV_HEADS, HEAD_DIM), (1, 0, 2))
    grouped = lax.map(one_group, (q_stack, k_stack, v_stack))
    attn = jnp.transpose(grouped, (1, 0, 2, 3)).reshape(seq_len, HEADS * HEAD_DIM)
    projected = jnp.dot(attn, out_weight, preferred_element_type=jnp.float32)
    attended = (tokens.astype(jnp.float32) + projected).astype(jnp.bfloat16)
    attended_wide = attended.astype(jnp.float32)
    inverse_rms = lax.rsqrt(lax.optimization_barrier(jnp.mean(attended_wide * attended_wide, axis=1, keepdims=True)) + 1e-05)
    normed = (attended_wide * inverse_rms * norm_gain.astype(jnp.float32)).astype(jnp.bfloat16)
    gate_sum = jnp.dot(normed, gate_weight, preferred_element_type=jnp.float32)
    up_sum = jnp.dot(normed, up_weight, preferred_element_type=jnp.float32)
    hidden = (jax.nn.silu(gate_sum) * up_sum).astype(jnp.bfloat16)
    block_width = FF // N_TP
    hidden_blocks = jnp.transpose(hidden.reshape(seq_len, N_TP, block_width), (1, 0, 2))
    down_blocks = down_weight.reshape(N_TP, block_width, D)

    def add_block(total, pair):
        hidden_block, down_block = pair
        partial_value = jnp.dot(hidden_block, down_block, preferred_element_type=jnp.float32).astype(jnp.bfloat16)
        partial_value = lax.optimization_barrier(partial_value)
        return (total + partial_value.astype(jnp.float32), None)
    ffn_part, _ = lax.scan(add_block, jnp.zeros((seq_len, D), jnp.float32), (hidden_blocks, down_blocks))
    layer_out = (attended_wide + ffn_part).astype(jnp.bfloat16)
    return (attended, layer_out)
```

```python
import functools
import math

import jax
import jax.numpy as jnp
from jax import lax
from jax.experimental import pallas as pl
from jax.experimental.pallas import tpu as pltpu
from jax.sharding import PartitionSpec as P

MESH = pl.DeviceIdType.MESH
HEAD_DIM = 128
KEY_CHUNK = 512
LOG2_SCALE = HEAD_DIM ** (-0.5) * math.log2(math.e)
norm_eps = 1e-05

GATE, UP, DOWN = 0, 1, 2


def layer_kernel(
    sp_count, tp_count,
    tok_ref, gain_ref, q_hbm, k_hbm, v_hbm, wo_hbm, gate_hbm, up_hbm, down_hbm,
    att_ref, out_ref,
    kv_all, q_all, qt_ref, acc_ref, attn_out, attn_full, wo_full, rows_all,
    gate_full, up_full, down_full, pair_buf, rs_buf,
    loc, kvz_s, kvz_r, qz_s, qz_r, woz_s, woz_r, az_s, az_r,
    pk_s, pk_r, pkf_s, pkf_r, pw_s, pw_r, pwf_s, pwf_r, pr_s, pr_r, prf_s, prf_r,
    w_s, w_r, pair_s, pair_r, rs_s, rs_r,
):
    S, T = sp_count, tp_count
    half = T // 2
    rows, D = tok_ref.shape
    HG = q_hbm.shape[1] // S
    KG = k_hbm.shape[1] // S
    DG = D // S
    WC = wo_hbm.shape[1]
    F = gate_hbm.shape[1]
    kv_local = KG // HEAD_DIM
    group = HG // KG
    width = group * rows
    segment_len = T * rows
    s = lax.axis_index("sp")
    t = lax.axis_index("tp")
    parity = lax.rem(t, 2)
    partner = t + 1 - 2 * parity

    def zpeer(d):
        return lax.rem(s + d, S)

    def tpeer(c):
        return lax.rem(t + 2 * c, T)

    def al(x, m):
        return pl.multiple_of(x, m)

    barrier = pltpu.get_barrier_semaphore()
    for d in range(1, S):
        pl.semaphore_signal(barrier, inc=1, device_id=(zpeer(d), t), device_id_type=MESH)
    for c in range(1, T):
        pl.semaphore_signal(
            barrier, inc=1, device_id=(s, lax.rem(t + c, T)), device_id_type=MESH
        )
    pl.semaphore_wait(barrier, S - 1 + T - 1)

    def remote(src, dst, ssem, rsem, ds, dt):
        return pltpu.make_async_remote_copy(
            src_ref=src, dst_ref=dst, send_sem=ssem, recv_sem=rsem,
            device_id=(ds, dt), device_id_type=MESH,
        )

    def kv_block(g, tt):
        return kv_all.at[pl.ds(al((g * T + tt) * rows, rows), rows), :]

    def kv_part(g, i):
        return kv_all.at[pl.ds(al((g * T + t) * rows, rows), rows), pl.ds(i * KG, KG)]

    def wo_piece(j):
        return wo_full.at[pl.ds(al(j * HG, HG), HG), pl.ds(al(t * WC, WC), WC)]

    def wo_block(tt):
        return wo_full.at[:, pl.ds(al(tt * WC, WC), WC)]

    def row_block(tt):
        return rows_all.at[pl.ds(al(tt * rows, rows), rows), :]

    fulls = (gate_full, up_full, down_full)
    owns = (gate_hbm, up_hbm, down_hbm)

    def w_slice(m, j):
        if m == DOWN:
            return down_full.at[:, pl.ds(al(j * DG, DG), DG)]
        return fulls[m].at[pl.ds(al(j * DG, DG), DG), :]

    def kvz(d, i):
        src = (k_hbm, v_hbm)[i].at[:, pl.ds(al(zpeer(d) * KG, KG), KG)]
        return remote(src, kv_part(s, i), kvz_s.at[d - 1, i], kvz_r.at[d - 1, i], zpeer(d), t)

    def qz(d):
        src = q_hbm.at[:, pl.ds(al(zpeer(d) * HG, HG), HG)]
        return remote(src, q_all.at[s], qz_s.at[d - 1], qz_r.at[d - 1], zpeer(d), t)

    def woz(d):
        return remote(wo_hbm, wo_piece(s), woz_s.at[d - 1], woz_r.at[d - 1], zpeer(d), t)

    kv_loc = [
        pltpu.make_async_copy(
            (k_hbm, v_hbm)[i].at[:, pl.ds(al(s * KG, KG), KG)], kv_part(s, i), loc.at[i]
        )
        for i in range(2)
    ]
    q_loc = pltpu.make_async_copy(
        q_hbm.at[:, pl.ds(al(s * HG, HG), HG)], q_all.at[s], loc.at[2]
    )
    wo_loc = pltpu.make_async_copy(wo_hbm, wo_piece(s), loc.at[3])
    w_loc = [
        pltpu.make_async_copy(owns[m], w_slice(m, s), loc.at[4 + m]) for m in range(3)
    ]

    def w_copy(m, d, side):
        j = s - d if side == 0 else s + d
        to = s + 1 if side == 0 else s - 1
        src = owns[m] if d == 0 else w_slice(m, j)
        return remote(src, w_slice(m, j), w_s.at[m, d, side], w_r.at[m, d, side], to, t)

    def w_sends(m, d, act):
        @pl.when(jnp.logical_and(s - d >= 0, s + 1 < S))
        def _():
            act(w_copy(m, d, 0))

        @pl.when(jnp.logical_and(s + d < S, s >= 1))
        def _():
            act(w_copy(m, d, 1))

    def w_wait(m, d):
        @pl.when(s - d >= 0)
        def _():
            j = s - d
            remote(
                w_slice(m, j), w_slice(m, j), w_s.at[m, d - 1, 0], w_r.at[m, d - 1, 0], s - 1, t
            ).wait_recv()

        @pl.when(s + d < S)
        def _():
            j = s + d
            remote(
                w_slice(m, j), w_slice(m, j), w_s.at[m, d - 1, 1], w_r.at[m, d - 1, 1], s + 1, t
            ).wait_recv()

    def start(copy):
        copy.start()

    for c in kv_loc:
        c.start()
    q_loc.start()
    wo_loc.start()
    for d in range(1, S):
        for i in range(2):
            kvz(d, i).start()
    for d in range(1, S):
        qz(d).start()
    for d in range(1, S):
        woz(d).start()
    for c in w_loc:
        c.start()
    for m in (GATE, UP, DOWN):
        w_sends(m, 0, start)

    def plane_send(block, ss, rs_, fs, fr):
        for c in range(1, half):
            remote(block(t), block(t), ss(c - 1), rs_(c - 1), s, tpeer(c)).start()
        remote(block(t), block(t), fs(0), fr(0), s, partner).start()

    def plane_forward(block, ss, rs_, fs, fr):
        for c in range(1, half):
            src = lax.rem(t - 2 * c + 2 * T, T)
            remote(block(src), block(src), ss(c - 1), rs_(c - 1), s, src).wait_recv()
            remote(block(src), block(src), fs(c), fr(c), s, partner).start()

    def plane_wait(block, ss, rs_, fs, fr):
        for c in range(half):
            src = lax.rem(partner - 2 * c + 2 * T, T)
            remote(block(src), block(src), fs(c), fr(c), s, partner).wait_recv()

    def plane_drain(block, ss, rs_, fs, fr):
        for c in range(1, half):
            remote(block(t), block(t), ss(c - 1), rs_(c - 1), s, tpeer(c)).wait_send()
        for c in range(half):
            remote(block(t), block(t), fs(c), fr(c), s, partner).wait_send()

    def kv_plane(g):
        return (
            lambda tt: kv_block(g, tt),
            lambda c: pk_s.at[g, c], lambda c: pk_r.at[g, c],
            lambda c: pkf_s.at[g, c], lambda c: pkf_r.at[g, c],
        )

    wo_plane = (
        wo_block,
        lambda c: pw_s.at[c], lambda c: pw_r.at[c],
        lambda c: pwf_s.at[c], lambda c: pwf_r.at[c],
    )
    row_plane = (
        row_block,
        lambda c: pr_s.at[c], lambda c: pr_r.at[c],
        lambda c: prf_s.at[c], lambda c: prf_r.at[c],
    )

    for c in kv_loc:
        c.wait()
    plane_send(*kv_plane(s))
    for g in range(S):
        @pl.when(s != g)
        def _():
            d = lax.rem(s - g + S, S)
            for i in range(2):
                remote(
                    kv_part(g, i), kv_part(g, i), kvz_s.at[d - 1, i], kvz_r.at[d - 1, i], g, t
                ).wait_recv()
            plane_send(*kv_plane(g))

    def attention(g):
        first_row = g * segment_len + t * rows
        for h in range(kv_local):
            for e in range(group):
                head = h * group + e
                qt_ref[h, :, e * rows : (e + 1) * rows] = q_all[
                    g, :, head * HEAD_DIM : (head + 1) * HEAD_DIM
                ].T
        acc_ref[...] = jnp.zeros_like(acc_ref)

        def step(chunk, carry, masked):
            first = al(chunk * KEY_CHUNK, KEY_CHUNK)
            scores = []
            for h in range(kv_local):
                k = kv_all[pl.ds(first, KEY_CHUNK), h * HEAD_DIM : (h + 1) * HEAD_DIM]
                sc = jnp.dot(k, qt_ref[h], preferred_element_type=jnp.float32)
                if masked:
                    key_pos = first + lax.broadcasted_iota(jnp.int32, (KEY_CHUNK, width), 0)
                    lane = lax.broadcasted_iota(jnp.int32, (KEY_CHUNK, width), 1)
                    sc = jnp.where(key_pos <= first_row + lax.rem(lane, rows), sc, -1e30)
                scores.append(sc)
            result = []
            for h in range(kv_local):
                peak, total = carry[h]
                sc = scores[h]
                new_peak = jnp.maximum(peak, jnp.max(sc, axis=0, keepdims=True))
                p = jnp.exp2((sc - new_peak) * LOG2_SCALE)
                fade = jnp.exp2((peak - new_peak) * LOG2_SCALE)
                total = total * fade + jnp.sum(p, axis=0, keepdims=True)
                v_at = KG + h * HEAD_DIM
                v = kv_all[pl.ds(first, KEY_CHUNK), v_at : v_at + HEAD_DIM]
                acc_ref[h] = acc_ref[h] * fade + lax.dot_general(
                    v, p.astype(jnp.bfloat16), (((0,), (0,)), ((), ())),
                    preferred_element_type=jnp.float32,
                )
                result.append((new_peak, total))
            return tuple(result)

        carry = tuple(
            (jnp.full((1, width), -1e30, jnp.float32), jnp.zeros((1, width), jnp.float32))
            for _ in range(kv_local)
        )
        whole_chunks = first_row // KEY_CHUNK
        carry = lax.fori_loop(0, whole_chunks, lambda i, c: step(i, c, False), carry)
        carry = step(whole_chunks, carry, True)
        for h in range(kv_local):
            mixed = (acc_ref[h] / carry[h][1]).astype(jnp.bfloat16)
            for e in range(group):
                head = h * group + e
                attn_out[g, :, head * HEAD_DIM : (head + 1) * HEAD_DIM] = mixed[
                    :, e * rows : (e + 1) * rows
                ].T

    def attn_copy(g):
        d = lax.rem(g - s + S, S)
        return remote(
            attn_out.at[g], attn_full.at[:, pl.ds(al(s * HG, HG), HG)],
            az_s.at[d - 1], az_r.at[d - 1], g, t,
        )

    def wo_z_wait():
        wo_loc.wait()
        for d in range(1, S):
            src = lax.rem(s - d + S, S)
            remote(wo_piece(src), wo_piece(src), woz_s.at[d - 1], woz_r.at[d - 1], src, t).wait_recv()

    plane_forward(*kv_plane(0))
    for g in range(S):
        if g + 1 < S:
            plane_forward(*kv_plane(g + 1))
        if g == min(1, S - 1):
            wo_z_wait()
            plane_send(*wo_plane)
        if g == S - 1:
            plane_forward(*wo_plane)

        @pl.when(s == g)
        def _():
            q_loc.wait()

        @pl.when(s != g)
        def _():
            d = lax.rem(s - g + S, S)
            remote(q_all.at[g], q_all.at[g], qz_s.at[d - 1], qz_r.at[d - 1], g, t).wait_recv()

        plane_wait(*kv_plane(g))
        attention(g)

        @pl.when(s == g)
        def _():
            attn_full[:, pl.ds(al(s * HG, HG), HG)] = attn_out[g]

        @pl.when(s != g)
        def _():
            attn_copy(g).start()

    for m in (GATE, UP):
        if S > 1:
            w_wait(m, 1)
        if S > 2:
            w_sends(m, 1, start)

    plane_wait(*wo_plane)
    for d in range(1, S):
        src = lax.rem(s - d + S, S)
        piece = attn_full.at[:, pl.ds(al(src * HG, HG), HG)]
        remote(piece, piece, az_s.at[d - 1], az_r.at[d - 1], src, t).wait_recv()

    tile = DG

    def project(n, squares):
        at = pl.ds(al(n * tile, tile), tile)
        total = jnp.dot(attn_full[...], wo_full[:, at], preferred_element_type=jnp.float32)
        a = (tok_ref[:, at].astype(jnp.float32) + total).astype(jnp.bfloat16)
        att_ref[:, at] = a
        wide = a.astype(jnp.float32)
        return squares + jnp.sum(wide * wide, axis=1, keepdims=True)

    squares = lax.fori_loop(0, S, project, jnp.zeros((rows, 1), jnp.float32))
    inverse_rms = lax.rsqrt(squares * (1.0 / D) + norm_eps)
    my_rows = pl.ds(al(t * rows, rows), rows)
    rows_all[my_rows, :] = (
        att_ref[...].astype(jnp.float32) * inverse_rms * gain_ref[...].astype(jnp.float32)
    ).astype(jnp.bfloat16)
    plane_send(*row_plane)

    for d in range(2, S - 1):
        for m in (GATE, UP):
            w_wait(m, d)
            w_sends(m, d, start)
    if S > 1:
        w_wait(DOWN, 1)
    if S > 2:
        w_sends(DOWN, 1, start)
    plane_forward(*row_plane)
    if S > 2:
        for m in (GATE, UP):
            w_wait(m, S - 1)
    w_loc[GATE].wait()
    w_loc[UP].wait()
    plane_wait(*row_plane)
    plane_drain(*wo_plane)
    for g in range(S):
        plane_drain(*kv_plane(g))

    step_rows = 2 * rows

    def hidden_step(b, _):
        at = pl.ds(al(b * step_rows, step_rows), step_rows)
        x = rows_all[at, :]
        gate = jnp.dot(x, gate_full[...], preferred_element_type=jnp.float32)
        up = jnp.dot(x, up_full[...], preferred_element_type=jnp.float32)
        wo_full[at, :F] = (gate / (1.0 + jnp.exp(-gate)) * up).astype(jnp.bfloat16)
        return 0

    lax.fori_loop(0, half, hidden_step, 0)

    near = jnp.minimum(s, S - 1 - s)

    def order(k):
        far = (k + 1) // 2
        swing = s - far if k % 2 else s + far
        tail = jnp.where(s == near, k, S - 1 - k)
        return jnp.where(k <= 2 * near, swing, tail)

    mine_base = S * half * rows

    def region(j, own):
        base = jnp.where(own, mine_base, 0)
        return base + j * (half * rows)

    def pair_copy(j):
        src = kv_all.at[pl.ds(al(region(j, False), rows), half * rows), :]
        return remote(src, pair_buf.at[j], pair_s.at[j], pair_r.at[j], s, partner)

    def rs_copy(j, c):
        block = lax.rem(t // 2 + c, half)
        src = kv_all.at[pl.ds(al(region(j, True) + block * rows, rows), rows), :]
        return remote(src, rs_buf.at[j, c - 1], rs_s.at[j, c - 1], rs_r.at[j, c - 1], s, tpeer(c))

    def down_step(j):
        cols = pl.ds(al(j * DG, DG), DG)

        def body(b, _):
            at = pl.ds(al(b * step_rows, step_rows), step_rows)
            y = jnp.dot(wo_full[at, :F], down_full[:, cols], preferred_element_type=jnp.float32)
            y = y.astype(jnp.bfloat16)
            for e in range(2):
                to = region(j, parity == e) + b * rows
                kv_all[pl.ds(al(to, rows), rows), :] = y[e * rows : (e + 1) * rows]
            return 0

        lax.fori_loop(0, half, body, 0)
        pair_copy(j).start()

    def reduce_step(j):
        pair_copy(j).wait_recv()
        for c in range(1, half):
            block = lax.rem(t // 2 + c, half)
            at = pl.ds(al(region(j, True) + block * rows, rows), rows)
            other = pair_buf[j, pl.ds(al(block * rows, rows), rows), :]
            kv_all[at, :] = (
                kv_all[at, :].astype(jnp.float32) + other.astype(jnp.float32)
            ).astype(jnp.bfloat16)
            rs_copy(j, c).start()

    w_loc[DOWN].wait()
    for k in range(S):
        j = order(k)
        dist = jnp.where(j < s, s - j, j - s)
        if k >= 1:
            for d in range(2, S):
                @pl.when(jnp.logical_and(dist == d, j < s))
                def _():
                    remote(
                        w_slice(DOWN, s - d), w_slice(DOWN, s - d),
                        w_s.at[DOWN, d - 1, 0], w_r.at[DOWN, d - 1, 0], s - 1, t,
                    ).wait_recv()
                    if d < S - 1:
                        @pl.when(s + 1 < S)
                        def _():
                            w_copy(DOWN, d, 0).start()

                @pl.when(jnp.logical_and(dist == d, j > s))
                def _():
                    remote(
                        w_slice(DOWN, s + d), w_slice(DOWN, s + d),
                        w_s.at[DOWN, d - 1, 1], w_r.at[DOWN, d - 1, 1], s + 1, t,
                    ).wait_recv()
                    if d < S - 1:
                        @pl.when(s >= 1)
                        def _():
                            w_copy(DOWN, d, 1).start()
        down_step(j)
        if k >= 1:
            reduce_step(order(k - 1))
    reduce_step(order(S - 1))

    mine = t // 2
    for k in range(S):
        j = order(k)
        cols = pl.ds(al(j * DG, DG), DG)
        for c in range(1, half):
            rs_copy(j, c).wait_recv()
        at = pl.ds(al(region(j, True) + mine * rows, rows), rows)
        total = att_ref[:, cols].astype(jnp.float32)
        total += kv_all[at, :].astype(jnp.float32)
        total += pair_buf[j, pl.ds(al(mine * rows, rows), rows), :].astype(jnp.float32)
        for c in range(1, half):
            total += rs_buf[j, c - 1].astype(jnp.float32)
        out_ref[:, cols] = total.astype(jnp.bfloat16)

    for d in range(1, S):
        for i in range(2):
            kvz(d, i).wait_send()
        qz(d).wait_send()
        woz(d).wait_send()
    for g in range(S):
        @pl.when(s != g)
        def _():
            attn_copy(g).wait_send()
    for m in (GATE, UP, DOWN):
        for d in range(S - 1):
            w_sends(m, d, lambda copy: copy.wait_send())
    plane_drain(*row_plane)
    for j in range(S):
        pair_copy(j).wait_send()
        for c in range(1, half):
            rs_copy(j, c).wait_send()


def shards(
    tokens, queries, keys, values, out_weight, norm_gain, gate_weight, up_weight, down_weight
):
    S = lax.axis_size("sp")
    T = lax.axis_size("tp")
    rows, D = tokens.shape
    HG = queries.shape[1] // S
    KG = keys.shape[1] // S
    DG = D // S
    F = gate_weight.shape[1]
    half = T // 2
    kv_local = KG // HEAD_DIM
    width = HG // KG * rows
    assert T % 2 == 0 and 2 * KG == DG and T * rows == S * HG and F <= D
    bf16, f32 = jnp.bfloat16, jnp.float32
    vmem, any_ = pl.BlockSpec(memory_space=pltpu.VMEM), pl.BlockSpec(memory_space=pl.ANY)
    sem = pltpu.SemaphoreType.DMA
    line = S - 1
    return pl.pallas_call(
        functools.partial(layer_kernel, S, T),
        out_shape=(
            jax.ShapeDtypeStruct((rows, D), bf16),
            jax.ShapeDtypeStruct((rows, D), bf16),
        ),
        in_specs=[vmem, vmem] + [any_] * 7,
        out_specs=(vmem, vmem),
        scratch_shapes=[
            pltpu.VMEM((S * T * rows, 2 * KG), bf16),
            pltpu.VMEM((S, rows, HG), bf16),
            pltpu.VMEM((kv_local, HEAD_DIM, width), bf16),
            pltpu.VMEM((kv_local, HEAD_DIM, width), f32),
            pltpu.VMEM((S, rows, HG), bf16),
            pltpu.VMEM((rows, S * HG), bf16),
            pltpu.VMEM((S * HG, D), bf16),
            pltpu.VMEM((T * rows, D), bf16),
            pltpu.VMEM((D, F), bf16),
            pltpu.VMEM((D, F), bf16),
            pltpu.VMEM((F, D), bf16),
            pltpu.VMEM((S, half * rows, DG), bf16),
            pltpu.VMEM((S, half - 1, rows, DG), bf16),
            sem((7,)),
            sem((line, 2)), sem((line, 2)), sem((line,)), sem((line,)),
            sem((line,)), sem((line,)), sem((line,)), sem((line,)),
            sem((S, half - 1)), sem((S, half - 1)), sem((S, half)), sem((S, half)),
            sem((half - 1,)), sem((half - 1,)), sem((half,)), sem((half,)),
            sem((half - 1,)), sem((half - 1,)), sem((half,)), sem((half,)),
            sem((3, line, 2)), sem((3, line, 2)),
            sem((S,)), sem((S,)), sem((S, half - 1)), sem((S, half - 1)),
        ],
        compiler_params=pltpu.CompilerParams(
            collective_id=0,
            has_side_effects=True,
            vmem_limit_bytes=67_043_328,
        ),
    )(
        tokens, norm_gain.reshape(1, D), queries, keys, values, out_weight,
        gate_weight, up_weight, down_weight,
    )


def solution(mesh):
    return jax.shard_map(
        shards,
        mesh=mesh,
        in_specs=(
            P(("sp", "tp"), None),
            P(("sp", "tp"), None),
            P(("sp", "tp"), None),
            P(("sp", "tp"), None),
            P("sp", "tp"),
            P(),
            P("sp", "tp"),
            P("sp", "tp"),
            P("tp", "sp"),
        ),
        out_specs=(P(("sp", "tp"), None), P(("sp", "tp"), None)),
        check_vma=False,
    )
```

```python
import functools
import math

import jax
import jax.numpy as jnp
from jax import lax
from jax.experimental import pallas as pl
from jax.experimental.pallas import tpu as pltpu
from jax.sharding import PartitionSpec as P

MESH = pl.DeviceIdType.MESH
HEAD_DIM = 128
KEY_CHUNK = 512
LOG2_SCALE = HEAD_DIM ** (-0.5) * math.log2(math.e)
norm_eps = 1e-05

GATE, UP, DOWN = 0, 1, 2
PARTS = 4
LAG = 5


def parts_of(columns):
    return min(PARTS, columns // 128)


def layer_kernel(
    sp_count, tp_count,
    tok_ref, gain_ref, q_hbm, k_hbm, v_hbm, wo_hbm, gate_hbm, up_hbm, down_hbm,
    att_ref, out_ref,
    kv_all, q_all, qt_ref, acc_ref, attn_out, attn_full, wo_full, rows_all,
    gate_full, up_full, down_full, pair_buf, rs_buf,
    loc, kvz_s, kvz_r, qz_s, qz_r, woz_s, woz_r, az_s, az_r,
    pk_s, pk_r, pkf_s, pkf_r, pw_s, pw_r, pwf_s, pwf_r, pr_s, pr_r, prf_s, prf_r,
    w_s, w_r, pair_s, pair_r, rs_s, rs_r,
):
    S, T = sp_count, tp_count
    half = T // 2
    rows, D = tok_ref.shape
    HG = q_hbm.shape[1] // S
    KG = k_hbm.shape[1] // S
    DG = D // S
    SUB = parts_of(DG)
    SW = DG // SUB
    WC = wo_hbm.shape[1]
    F = gate_hbm.shape[1]
    kv_local = KG // HEAD_DIM
    group = HG // KG
    width = group * rows
    segment_len = T * rows
    s = lax.axis_index("sp")
    t = lax.axis_index("tp")
    parity = lax.rem(t, 2)
    partner = t + 1 - 2 * parity

    def zpeer(d):
        return lax.rem(s + d, S)

    def tpeer(c):
        return lax.rem(t + 2 * c, T)

    def al(x, m):
        return pl.multiple_of(x, m)

    barrier = pltpu.get_barrier_semaphore()
    for d in range(1, S):
        pl.semaphore_signal(barrier, inc=1, device_id=(zpeer(d), t), device_id_type=MESH)
    for c in range(1, T):
        pl.semaphore_signal(
            barrier, inc=1, device_id=(s, lax.rem(t + c, T)), device_id_type=MESH
        )
    pl.semaphore_wait(barrier, S - 1 + T - 1)

    def remote(src, dst, ssem, rsem, ds, dt):
        return pltpu.make_async_remote_copy(
            src_ref=src, dst_ref=dst, send_sem=ssem, recv_sem=rsem,
            device_id=(ds, dt), device_id_type=MESH,
        )

    def kv_block(g, tt):
        return kv_all.at[pl.ds(al((g * T + tt) * rows, rows), rows), :]

    def kv_part(g, i):
        return kv_all.at[pl.ds(al((g * T + t) * rows, rows), rows), pl.ds(i * KG, KG)]

    def wo_piece(j):
        return wo_full.at[pl.ds(al(j * HG, HG), HG), pl.ds(al(t * WC, WC), WC)]

    def wo_block(tt):
        return wo_full.at[:, pl.ds(al(tt * WC, WC), WC)]

    def row_block(tt):
        return rows_all.at[pl.ds(al(tt * rows, rows), rows), :]

    def w_own(m):
        if m >= DOWN:
            return down_hbm.at[:, pl.ds((m - DOWN) * SW, SW)]
        return (gate_hbm, up_hbm)[m]

    def w_slice(m, j):
        if m >= DOWN:
            return down_full.at[:, pl.ds(al(j * DG + (m - DOWN) * SW, SW), SW)]
        return (gate_full, up_full)[m].at[pl.ds(al(j * DG, DG), DG), :]

    def kvz(d, i):
        src = (k_hbm, v_hbm)[i].at[:, pl.ds(al(zpeer(d) * KG, KG), KG)]
        return remote(src, kv_part(s, i), kvz_s.at[d - 1, i], kvz_r.at[d - 1, i], zpeer(d), t)

    def qz(d):
        src = q_hbm.at[:, pl.ds(al(zpeer(d) * HG, HG), HG)]
        return remote(src, q_all.at[s], qz_s.at[d - 1], qz_r.at[d - 1], zpeer(d), t)

    def woz(d):
        return remote(wo_hbm, wo_piece(s), woz_s.at[d - 1], woz_r.at[d - 1], zpeer(d), t)

    kv_loc = [
        pltpu.make_async_copy(
            (k_hbm, v_hbm)[i].at[:, pl.ds(al(s * KG, KG), KG)], kv_part(s, i), loc.at[i]
        )
        for i in range(2)
    ]
    q_loc = pltpu.make_async_copy(
        q_hbm.at[:, pl.ds(al(s * HG, HG), HG)], q_all.at[s], loc.at[2]
    )
    wo_loc = pltpu.make_async_copy(wo_hbm, wo_piece(s), loc.at[3])
    w_loc = [
        pltpu.make_async_copy(w_own(m), w_slice(m, s), loc.at[4 + m]) for m in range(2 + SUB)
    ]

    def w_copy(m, d, side):
        j = s - d if side == 0 else s + d
        to = s + 1 if side == 0 else s - 1
        src = w_own(m) if d == 0 else w_slice(m, j)
        return remote(src, w_slice(m, j), w_s.at[m, d, side], w_r.at[m, d, side], to, t)

    def w_sends(m, d, act):
        @pl.when(jnp.logical_and(s - d >= 0, s + 1 < S))
        def _():
            act(w_copy(m, d, 0))

        @pl.when(jnp.logical_and(s + d < S, s >= 1))
        def _():
            act(w_copy(m, d, 1))

    def w_arrival(m, d, side):
        j = s - d if side == 0 else s + d
        sender = s - 1 if side == 0 else s + 1
        return remote(
            w_slice(m, j), w_slice(m, j),
            w_s.at[m, d - 1, side], w_r.at[m, d - 1, side], sender, t,
        )

    def w_pass(m, d):
        @pl.when(jnp.logical_and(s - d >= 0, s + 1 < S))
        def _():
            if d > 0:
                w_arrival(m, d, 0).wait_recv()
            w_copy(m, d, 0).start()

        @pl.when(jnp.logical_and(s + d < S, s >= 1))
        def _():
            if d > 0:
                w_arrival(m, d, 1).wait_recv()
            w_copy(m, d, 1).start()

    def w_rest(m, d):
        @pl.when(s == S - 1)
        def _():
            w_arrival(m, d, 0).wait_recv()

        @pl.when(s == 0)
        def _():
            w_arrival(m, d, 1).wait_recv()

    for c in kv_loc:
        c.start()
    q_loc.start()
    wo_loc.start()
    for d in range(1, S):
        for i in range(2):
            kvz(d, i).start()
    for d in range(1, S):
        qz(d).start()
    for c in w_loc:
        c.start()

    square = half == 4
    tx = t + 2 - 4 * lax.rem(t // 2, 2)
    ty = t + 4 - 8 * lax.rem(t // 4, 2)
    td = tx + ty - t
    if square:
        sources = (t, tx, ty, td)
    else:
        sources = tuple(lax.rem(t - 2 * c + 2 * T, T) for c in range(half))

    def part_of(block, i):
        size = block.shape[0] // 2
        return block.at[pl.ds(i * size, size), :]

    def plane_send(block, ss, rs_, fs, fr):
        if square:
            remote(block(t), block(t), ss(0), rs_(0), s, tx).start()
            remote(block(t), block(t), ss(1), rs_(1), s, ty).start()
        else:
            for c in range(1, half):
                remote(block(t), block(t), ss(c - 1), rs_(c - 1), s, tpeer(c)).start()
        remote(block(t), block(t), fs(0), fr(0), s, partner).start()

    def plane_forward(block, ss, rs_, fs, fr):
        if square:
            for i, (src, to) in enumerate(((tx, ty), (ty, tx))):
                remote(block(src), block(src), ss(i), rs_(i), s, src).wait_recv()
                piece = part_of(block(src), i)
                remote(piece, piece, ss(2 + i), rs_(2 + i), s, to).start()
                remote(block(src), block(src), fs(1 + i), fr(1 + i), s, partner).start()
            return
        for c in range(1, half):
            src = sources[c]
            remote(block(src), block(src), ss(c - 1), rs_(c - 1), s, src).wait_recv()
            remote(block(src), block(src), fs(c), fr(c), s, partner).start()

    def plane_corner(block, ss, rs_, fs, fr):
        if square:
            for i, src in enumerate((ty, tx)):
                piece = part_of(block(td), i)
                remote(piece, piece, ss(2 + i), rs_(2 + i), s, src).wait_recv()
            remote(block(td), block(td), fs(3), fr(3), s, partner).start()

    def plane_wait(block, ss, rs_, fs, fr):
        for c in range(half):
            src = sources[c] + partner - t if square else lax.rem(partner - 2 * c + 2 * T, T)
            remote(block(src), block(src), fs(c), fr(c), s, partner).wait_recv()

    def plane_drain(block, ss, rs_, fs, fr):
        if square:
            for i, to in enumerate((tx, ty)):
                remote(block(t), block(t), ss(i), rs_(i), s, to).wait_send()
            for i, to in enumerate((ty, tx)):
                piece = part_of(block(t), i)
                remote(piece, piece, ss(2 + i), rs_(2 + i), s, to).wait_send()
        else:
            for c in range(1, half):
                remote(block(t), block(t), ss(c - 1), rs_(c - 1), s, tpeer(c)).wait_send()
        for c in range(half):
            remote(block(t), block(t), fs(c), fr(c), s, partner).wait_send()

    def kv_plane(g):
        return (
            lambda tt: kv_block(g, tt),
            lambda c: pk_s.at[g, c], lambda c: pk_r.at[g, c],
            lambda c: pkf_s.at[g, c], lambda c: pkf_r.at[g, c],
        )

    wo_plane = (
        wo_block,
        lambda c: pw_s.at[c], lambda c: pw_r.at[c],
        lambda c: pwf_s.at[c], lambda c: pwf_r.at[c],
    )
    row_plane = (
        row_block,
        lambda c: pr_s.at[c], lambda c: pr_r.at[c],
        lambda c: prf_s.at[c], lambda c: prf_r.at[c],
    )

    for c in kv_loc:
        c.wait()
    plane_send(*kv_plane(s))
    for g in range(S):
        @pl.when(s != g)
        def _():
            d = lax.rem(s - g + S, S)
            for i in range(2):
                remote(
                    kv_part(g, i), kv_part(g, i), kvz_s.at[d - 1, i], kvz_r.at[d - 1, i], g, t
                ).wait_recv()
            plane_send(*kv_plane(g))

    def attention(g):
        first_row = g * segment_len + t * rows
        for h in range(kv_local):
            for e in range(group):
                head = h * group + e
                qt_ref[h, :, e * rows : (e + 1) * rows] = q_all[
                    g, :, head * HEAD_DIM : (head + 1) * HEAD_DIM
                ].T
        acc_ref[...] = jnp.zeros_like(acc_ref)

        def step(chunk, carry, masked):
            first = al(chunk * KEY_CHUNK, KEY_CHUNK)
            scores = []
            for h in range(kv_local):
                k = kv_all[pl.ds(first, KEY_CHUNK), h * HEAD_DIM : (h + 1) * HEAD_DIM]
                sc = jnp.dot(k, qt_ref[h], preferred_element_type=jnp.float32)
                if masked:
                    key_pos = first + lax.broadcasted_iota(jnp.int32, (KEY_CHUNK, width), 0)
                    lane = lax.broadcasted_iota(jnp.int32, (KEY_CHUNK, width), 1)
                    sc = jnp.where(key_pos <= first_row + lax.rem(lane, rows), sc, -1e30)
                scores.append(sc)
            result = []
            for h in range(kv_local):
                peak, total = carry[h]
                sc = scores[h]
                new_peak = jnp.maximum(peak, jnp.max(sc, axis=0, keepdims=True))
                p = jnp.exp2((sc - new_peak) * LOG2_SCALE)
                fade = jnp.exp2((peak - new_peak) * LOG2_SCALE)
                total = total * fade + jnp.sum(p, axis=0, keepdims=True)
                v_at = KG + h * HEAD_DIM
                v = kv_all[pl.ds(first, KEY_CHUNK), v_at : v_at + HEAD_DIM]
                acc_ref[h] = acc_ref[h] * fade + lax.dot_general(
                    v, p.astype(jnp.bfloat16), (((0,), (0,)), ((), ())),
                    preferred_element_type=jnp.float32,
                )
                result.append((new_peak, total))
            return tuple(result)

        carry = tuple(
            (jnp.full((1, width), -1e30, jnp.float32), jnp.zeros((1, width), jnp.float32))
            for _ in range(kv_local)
        )
        whole_chunks = first_row // KEY_CHUNK
        carry = lax.fori_loop(0, whole_chunks, lambda i, c: step(i, c, False), carry)
        carry = step(whole_chunks, carry, True)
        for h in range(kv_local):
            mixed = (acc_ref[h] / carry[h][1]).astype(jnp.bfloat16)
            for e in range(group):
                head = h * group + e
                attn_out[g, :, head * HEAD_DIM : (head + 1) * HEAD_DIM] = mixed[
                    :, e * rows : (e + 1) * rows
                ].T

    def attn_copy(g):
        d = lax.rem(g - s + S, S)
        return remote(
            attn_out.at[g], attn_full.at[:, pl.ds(al(s * HG, HG), HG)],
            az_s.at[d - 1], az_r.at[d - 1], g, t,
        )

    def wo_z_wait():
        wo_loc.wait()
        for d in range(1, S):
            src = lax.rem(s - d + S, S)
            remote(wo_piece(src), wo_piece(src), woz_s.at[d - 1], woz_r.at[d - 1], src, t).wait_recv()

    for d in range(1, S):
        woz(d).start()
    for m in (GATE, UP):
        w_pass(m, 0)
    plane_forward(*kv_plane(0))
    for g in range(S):
        if g + 1 < S:
            plane_forward(*kv_plane(g + 1))
        plane_corner(*kv_plane(g))
        if g == S - 1:
            wo_z_wait()
            plane_send(*wo_plane)

        @pl.when(s == g)
        def _():
            q_loc.wait()

        @pl.when(s != g)
        def _():
            d = lax.rem(s - g + S, S)
            remote(q_all.at[g], q_all.at[g], qz_s.at[d - 1], qz_r.at[d - 1], g, t).wait_recv()

        plane_wait(*kv_plane(g))
        attention(g)

        @pl.when(s == g)
        def _():
            attn_full[:, pl.ds(al(s * HG, HG), HG)] = attn_out[g]

        @pl.when(s != g)
        def _():
            attn_copy(g).start()

    plane_forward(*wo_plane)
    for m in (GATE, UP):
        if S > 2:
            w_pass(m, 1)
    plane_corner(*wo_plane)

    plane_wait(*wo_plane)
    for d in range(1, S):
        src = lax.rem(s - d + S, S)
        piece = attn_full.at[:, pl.ds(al(src * HG, HG), HG)]
        remote(piece, piece, az_s.at[d - 1], az_r.at[d - 1], src, t).wait_recv()

    tile = DG

    def project(n, squares):
        at = pl.ds(al(n * tile, tile), tile)
        total = jnp.dot(attn_full[...], wo_full[:, at], preferred_element_type=jnp.float32)
        a = (tok_ref[:, at].astype(jnp.float32) + total).astype(jnp.bfloat16)
        att_ref[:, at] = a
        wide = a.astype(jnp.float32)
        return squares + jnp.sum(wide * wide, axis=1, keepdims=True)

    squares = lax.fori_loop(0, S, project, jnp.zeros((rows, 1), jnp.float32))
    inverse_rms = lax.rsqrt(squares * (1.0 / D) + norm_eps)
    my_rows = pl.ds(al(t * rows, rows), rows)
    rows_all[my_rows, :] = (
        att_ref[...].astype(jnp.float32) * inverse_rms * gain_ref[...].reshape(1, D).astype(jnp.float32)
    ).astype(jnp.bfloat16)
    plane_send(*row_plane)

    for d in range(2, S - 1):
        w_pass(GATE, d)
        if d == 2:
            plane_forward(*row_plane)
        w_pass(UP, d)
    if S <= 3:
        plane_forward(*row_plane)
    for m in range(DOWN, DOWN + SUB):
        w_pass(m, 0)
    plane_corner(*row_plane)
    for d in range(1, S):
        for m in (GATE, UP):
            w_rest(m, d)
    w_loc[GATE].wait()
    w_loc[UP].wait()
    plane_wait(*row_plane)
    plane_drain(*wo_plane)
    for g in range(S):
        plane_drain(*kv_plane(g))

    step_rows = 2 * rows

    def hidden_step(b, _):
        at = pl.ds(al(b * step_rows, step_rows), step_rows)
        x = rows_all[at, :]
        gate = jnp.dot(x, gate_full[...], preferred_element_type=jnp.float32)
        up = jnp.dot(x, up_full[...], preferred_element_type=jnp.float32)
        wo_full[at, :F] = (gate / (1.0 + jnp.exp(-gate)) * up).astype(jnp.bfloat16)
        return 0

    lax.fori_loop(0, half, hidden_step, 0)

    near = jnp.minimum(s, S - 1 - s)

    def order(k):
        far = (k + 1) // 2
        swing = s - far if k % 2 else s + far
        tail = jnp.where(s == near, k, S - 1 - k)
        return jnp.where(k <= 2 * near, swing, tail)

    mine_base = S * half * rows

    def region(j, own):
        base = jnp.where(own, mine_base, 0)
        return base + j * (half * rows)

    def pair_copy(j, h):
        at = pl.ds(al(region(j, False), rows), half * rows)
        src = kv_all.at[at, pl.ds(h * SW, SW)]
        return remote(src, pair_buf.at[j, h], pair_s.at[j, h], pair_r.at[j, h], s, partner)

    def rs_copy(j, h, c):
        block = lax.rem(t // 2 + c, half)
        at = pl.ds(al(region(j, True) + block * rows, rows), rows)
        src = kv_all.at[at, pl.ds(h * SW, SW)]
        return remote(
            src, rs_buf.at[j, h, c - 1], rs_s.at[j, h, c - 1], rs_r.at[j, h, c - 1], s, tpeer(c)
        )

    def down_step(j, h):
        cols = pl.ds(al(j * DG + h * SW, SW), SW)

        def body(b, _):
            at = pl.ds(al(b * step_rows, step_rows), step_rows)
            y = jnp.dot(wo_full[at, :F], down_full[:, cols], preferred_element_type=jnp.float32)
            y = y.astype(jnp.bfloat16)
            for e in range(2):
                to = region(j, parity == e) + b * rows
                kv_all[pl.ds(al(to, rows), rows), h * SW : (h + 1) * SW] = y[
                    e * rows : (e + 1) * rows
                ]
            return 0

        lax.fori_loop(0, half, body, 0)
        pair_copy(j, h).start()

    def reduce_step(j, h):
        pair_copy(j, h).wait_recv()
        for c in range(1, half):
            block = lax.rem(t // 2 + c, half)
            at = pl.ds(al(region(j, True) + block * rows, rows), rows)
            cols = slice(h * SW, (h + 1) * SW)
            other = pair_buf[j, h, pl.ds(al(block * rows, rows), rows), :]
            kv_all[at, cols] = (
                kv_all[at, cols].astype(jnp.float32) + other.astype(jnp.float32)
            ).astype(jnp.bfloat16)
            rs_copy(j, h, c).start()

    mine = t // 2

    def finish(j, h):
        cols = pl.ds(al(j * DG + h * SW, SW), SW)
        for c in range(1, half):
            rs_copy(j, h, c).wait_recv()
        at = pl.ds(al(region(j, True) + mine * rows, rows), rows)
        total = att_ref[:, cols].astype(jnp.float32)
        total += kv_all[at, h * SW : (h + 1) * SW].astype(jnp.float32)
        total += pair_buf[j, h, pl.ds(al(mine * rows, rows), rows), :].astype(jnp.float32)
        for c in range(1, half):
            total += rs_buf[j, h, c - 1].astype(jnp.float32)
        out_ref[:, cols] = total.astype(jnp.bfloat16)

    steps = [(k, h) for k in range(S) for h in range(SUB)]
    for i, (k, h) in enumerate(steps):
        j = order(k)
        if h == 0 and 1 <= max(k, 1) < S - 1 and k != 1:
            for m in range(DOWN, DOWN + SUB):
                w_pass(m, max(k, 1))
        if k >= 1:
            w_rest(DOWN + h, k)
        elif h == 0:
            for m in range(DOWN, DOWN + SUB):
                w_loc[m].wait()
        down_step(j, h)
        if i >= 1:
            reduce_step(order(steps[i - 1][0]), steps[i - 1][1])
        if i >= LAG:
            finish(order(steps[i - LAG][0]), steps[i - LAG][1])
    k, h = steps[-1]
    reduce_step(order(k), h)
    for k, h in steps[max(len(steps) - LAG, 0):]:
        finish(order(k), h)

    for d in range(1, S):
        for i in range(2):
            kvz(d, i).wait_send()
        qz(d).wait_send()
        woz(d).wait_send()
    for g in range(S):
        @pl.when(s != g)
        def _():
            attn_copy(g).wait_send()
    for m in range(DOWN + SUB):
        for d in range(S - 1):
            w_sends(m, d, lambda copy: copy.wait_send())
    plane_drain(*row_plane)
    for j in range(S):
        for h in range(SUB):
            pair_copy(j, h).wait_send()
            for c in range(1, half):
                rs_copy(j, h, c).wait_send()


def shards(
    tokens, queries, keys, values, out_weight, norm_gain, gate_weight, up_weight, down_weight
):
    S = lax.axis_size("sp")
    T = lax.axis_size("tp")
    rows, D = tokens.shape
    HG = queries.shape[1] // S
    KG = keys.shape[1] // S
    DG = D // S
    F = gate_weight.shape[1]
    half = T // 2
    SUB = parts_of(DG)
    kv_local = KG // HEAD_DIM
    width = HG // KG * rows
    assert T % 2 == 0 and 2 * KG == DG and T * rows == S * HG and F <= D
    bf16, f32 = jnp.bfloat16, jnp.float32
    vmem, any_ = pl.BlockSpec(memory_space=pltpu.VMEM), pl.BlockSpec(memory_space=pl.ANY)
    sem = pltpu.SemaphoreType.DMA
    line = S - 1
    links = 4 if half == 4 else half - 1
    return pl.pallas_call(
        functools.partial(layer_kernel, S, T),
        out_shape=(
            jax.ShapeDtypeStruct((rows, D), bf16),
            jax.ShapeDtypeStruct((rows, D), bf16),
        ),
        in_specs=[vmem, vmem] + [any_] * 7,
        out_specs=(vmem, vmem),
        scratch_shapes=[
            pltpu.VMEM((S * T * rows, 2 * KG), bf16),
            pltpu.VMEM((S, rows, HG), bf16),
            pltpu.VMEM((kv_local, HEAD_DIM, width), bf16),
            pltpu.VMEM((kv_local, HEAD_DIM, width), f32),
            pltpu.VMEM((S, rows, HG), bf16),
            pltpu.VMEM((rows, S * HG), bf16),
            pltpu.VMEM((S * HG, D), bf16),
            pltpu.VMEM((T * rows, D), bf16),
            pltpu.VMEM((D, F), bf16),
            pltpu.VMEM((D, F), bf16),
            pltpu.VMEM((F, D), bf16),
            pltpu.VMEM((S, SUB, half * rows, DG // SUB), bf16),
            pltpu.VMEM((S, SUB, half - 1, rows, DG // SUB), bf16),
            sem((6 + SUB,)),
            sem((line, 2)), sem((line, 2)), sem((line,)), sem((line,)),
            sem((line,)), sem((line,)), sem((line,)), sem((line,)),
            sem((S, links)), sem((S, links)), sem((S, half)), sem((S, half)),
            sem((links,)), sem((links,)), sem((half,)), sem((half,)),
            sem((links,)), sem((links,)), sem((half,)), sem((half,)),
            sem((2 + SUB, line, 2)), sem((2 + SUB, line, 2)),
            sem((S, SUB)), sem((S, SUB)), sem((S, SUB, half - 1)), sem((S, SUB, half - 1)),
        ],
        compiler_params=pltpu.CompilerParams(
            collective_id=0,
            has_side_effects=True,
            vmem_limit_bytes=67_043_328,
        ),
    )(
        tokens, norm_gain, queries, keys, values, out_weight,
        gate_weight, up_weight, down_weight,
    )


def solution(mesh):
    return jax.shard_map(
        shards,
        mesh=mesh,
        in_specs=(
            P(("sp", "tp"), None),
            P(("sp", "tp"), None),
            P(("sp", "tp"), None),
            P(("sp", "tp"), None),
            P("sp", "tp"),
            P(),
            P("sp", "tp"),
            P("sp", "tp"),
            P("tp", "sp"),
        ),
        out_specs=(P(("sp", "tp"), None), P(("sp", "tp"), None)),
        check_vma=False,
    )
```

```python
import functools
import math

import jax
import jax.numpy as jnp
from jax import lax
from jax.experimental import pallas as pl
from jax.experimental.pallas import tpu as pltpu
from jax.sharding import PartitionSpec as P

MESH = pl.DeviceIdType.MESH
HEAD_DIM = 128
KEY_CHUNK = 512
LOG2_SCALE = HEAD_DIM ** (-0.5) * math.log2(math.e)
norm_eps = 1e-05

GATE, UP, DOWN = 0, 1, 2
PARTS = 4
LAG = 5


def parts_of(columns):
    return min(PARTS, columns // 128)


def layer_kernel(
    sp_count, tp_count,
    tok_ref, gain_ref, q_hbm, k_hbm, v_hbm, wo_hbm, gate_hbm, up_hbm, down_hbm,
    att_ref, out_ref,
    kv_all, q_all, qt_ref, acc_ref, attn_out, attn_full, wo_full, rows_all,
    gate_full, up_full, down_full, pair_buf, rs_buf, gate_sum,
    loc, kvz_s, kvz_r, qz_s, qz_r, woz_s, woz_r, az_s, az_r,
    pk_s, pk_r, pkf_s, pkf_r, pw_s, pw_r, pwf_s, pwf_r, pr_s, pr_r, prf_s, prf_r,
    w_s, w_r, pair_s, pair_r, rs_s, rs_r,
):
    S, T = sp_count, tp_count
    half = T // 2
    rows, D = tok_ref.shape
    HG = q_hbm.shape[1] // S
    KG = k_hbm.shape[1] // S
    DG = D // S
    SUB = parts_of(DG)
    SW = DG // SUB
    WC = wo_hbm.shape[1]
    F = gate_hbm.shape[1]
    kv_local = KG // HEAD_DIM
    group = HG // KG
    width = group * rows
    segment_len = T * rows
    s = lax.axis_index("sp")
    t = lax.axis_index("tp")
    parity = lax.rem(t, 2)
    partner = t + 1 - 2 * parity

    def zpeer(d):
        return lax.rem(s + d, S)

    def tpeer(c):
        return lax.rem(t + 2 * c, T)

    def al(x, m):
        return pl.multiple_of(x, m)

    barrier = pltpu.get_barrier_semaphore()
    for d in range(1, S):
        pl.semaphore_signal(barrier, inc=1, device_id=(zpeer(d), t), device_id_type=MESH)
    for c in range(1, T):
        pl.semaphore_signal(
            barrier, inc=1, device_id=(s, lax.rem(t + c, T)), device_id_type=MESH
        )
    pl.semaphore_wait(barrier, S - 1 + T - 1)

    def remote(src, dst, ssem, rsem, ds, dt):
        return pltpu.make_async_remote_copy(
            src_ref=src, dst_ref=dst, send_sem=ssem, recv_sem=rsem,
            device_id=(ds, dt), device_id_type=MESH,
        )

    def kv_block(g, tt):
        return kv_all.at[pl.ds(al((g * T + tt) * rows, rows), rows), :]

    def kv_part(g, i):
        return kv_all.at[pl.ds(al((g * T + t) * rows, rows), rows), pl.ds(i * KG, KG)]

    def wo_piece(j):
        return wo_full.at[pl.ds(al(j * HG, HG), HG), pl.ds(al(t * WC, WC), WC)]

    def wo_block(tt):
        return wo_full.at[:, pl.ds(al(tt * WC, WC), WC)]

    def row_block(tt):
        return rows_all.at[pl.ds(al(tt * rows, rows), rows), :]

    def w_own(m):
        if m >= DOWN:
            return down_hbm.at[:, pl.ds((m - DOWN) * SW, SW)]
        return (gate_hbm, up_hbm)[m]

    def w_slice(m, j):
        if m >= DOWN:
            return down_full.at[:, pl.ds(al(j * DG + (m - DOWN) * SW, SW), SW)]
        return (gate_full, up_full)[m].at[pl.ds(al(j * DG, DG), DG), :]

    def kvz(d, i):
        src = (k_hbm, v_hbm)[i].at[:, pl.ds(al(zpeer(d) * KG, KG), KG)]
        return remote(src, kv_part(s, i), kvz_s.at[d - 1, i], kvz_r.at[d - 1, i], zpeer(d), t)

    def qz(d):
        src = q_hbm.at[:, pl.ds(al(zpeer(d) * HG, HG), HG)]
        return remote(src, q_all.at[s], qz_s.at[d - 1], qz_r.at[d - 1], zpeer(d), t)

    def woz(d):
        return remote(wo_hbm, wo_piece(s), woz_s.at[d - 1], woz_r.at[d - 1], zpeer(d), t)

    kv_loc = [
        pltpu.make_async_copy(
            (k_hbm, v_hbm)[i].at[:, pl.ds(al(s * KG, KG), KG)], kv_part(s, i), loc.at[i]
        )
        for i in range(2)
    ]
    q_loc = pltpu.make_async_copy(
        q_hbm.at[:, pl.ds(al(s * HG, HG), HG)], q_all.at[s], loc.at[2]
    )
    wo_loc = pltpu.make_async_copy(wo_hbm, wo_piece(s), loc.at[3])
    w_loc = [
        pltpu.make_async_copy(w_own(m), w_slice(m, s), loc.at[4 + m]) for m in range(2 + SUB)
    ]

    def w_copy(m, d, side):
        j = s - d if side == 0 else s + d
        to = s + 1 if side == 0 else s - 1
        src = w_own(m) if d == 0 else w_slice(m, j)
        return remote(src, w_slice(m, j), w_s.at[m, d, side], w_r.at[m, d, side], to, t)

    def w_sends(m, d, act):
        @pl.when(jnp.logical_and(s - d >= 0, s + 1 < S))
        def _():
            act(w_copy(m, d, 0))

        @pl.when(jnp.logical_and(s + d < S, s >= 1))
        def _():
            act(w_copy(m, d, 1))

    def w_arrival(m, d, side):
        j = s - d if side == 0 else s + d
        sender = s - 1 if side == 0 else s + 1
        return remote(
            w_slice(m, j), w_slice(m, j),
            w_s.at[m, d - 1, side], w_r.at[m, d - 1, side], sender, t,
        )

    def w_pass(m, d):
        @pl.when(jnp.logical_and(s - d >= 0, s + 1 < S))
        def _():
            if d > 0:
                w_arrival(m, d, 0).wait_recv()
            w_copy(m, d, 0).start()

        @pl.when(jnp.logical_and(s + d < S, s >= 1))
        def _():
            if d > 0:
                w_arrival(m, d, 1).wait_recv()
            w_copy(m, d, 1).start()

    def w_rest(m, d):
        @pl.when(s == S - 1)
        def _():
            w_arrival(m, d, 0).wait_recv()

        @pl.when(s == 0)
        def _():
            w_arrival(m, d, 1).wait_recv()

    for c in kv_loc:
        c.start()
    q_loc.start()
    wo_loc.start()
    for d in range(1, S):
        for i in range(2):
            kvz(d, i).start()
    for d in range(1, S):
        qz(d).start()
    for c in w_loc:
        c.start()

    square = half == 4
    tx = t + 2 - 4 * lax.rem(t // 2, 2)
    ty = t + 4 - 8 * lax.rem(t // 4, 2)
    td = tx + ty - t
    if square:
        sources = (t, tx, ty, td)
    else:
        sources = tuple(lax.rem(t - 2 * c + 2 * T, T) for c in range(half))

    def part_of(block, i):
        size = block.shape[0] // 2
        return block.at[pl.ds(i * size, size), :]

    def plane_send(block, ss, rs_, fs, fr):
        if square:
            remote(block(t), block(t), ss(0), rs_(0), s, tx).start()
            remote(block(t), block(t), ss(1), rs_(1), s, ty).start()
        else:
            for c in range(1, half):
                remote(block(t), block(t), ss(c - 1), rs_(c - 1), s, tpeer(c)).start()
        remote(block(t), block(t), fs(0), fr(0), s, partner).start()

    def plane_forward(block, ss, rs_, fs, fr):
        if square:
            for i, (src, to) in enumerate(((tx, ty), (ty, tx))):
                remote(block(src), block(src), ss(i), rs_(i), s, src).wait_recv()
                piece = part_of(block(src), i)
                remote(piece, piece, ss(2 + i), rs_(2 + i), s, to).start()
                remote(block(src), block(src), fs(1 + i), fr(1 + i), s, partner).start()
            return
        for c in range(1, half):
            src = sources[c]
            remote(block(src), block(src), ss(c - 1), rs_(c - 1), s, src).wait_recv()
            remote(block(src), block(src), fs(c), fr(c), s, partner).start()

    def plane_corner(block, ss, rs_, fs, fr):
        if square:
            for i, src in enumerate((ty, tx)):
                piece = part_of(block(td), i)
                remote(piece, piece, ss(2 + i), rs_(2 + i), s, src).wait_recv()
            remote(block(td), block(td), fs(3), fr(3), s, partner).start()

    def plane_wait(block, ss, rs_, fs, fr):
        for c in range(half):
            src = sources[c] + partner - t if square else lax.rem(partner - 2 * c + 2 * T, T)
            remote(block(src), block(src), fs(c), fr(c), s, partner).wait_recv()

    def plane_drain(block, ss, rs_, fs, fr):
        if square:
            for i, to in enumerate((tx, ty)):
                remote(block(t), block(t), ss(i), rs_(i), s, to).wait_send()
            for i, to in enumerate((ty, tx)):
                piece = part_of(block(t), i)
                remote(piece, piece, ss(2 + i), rs_(2 + i), s, to).wait_send()
        else:
            for c in range(1, half):
                remote(block(t), block(t), ss(c - 1), rs_(c - 1), s, tpeer(c)).wait_send()
        for c in range(half):
            remote(block(t), block(t), fs(c), fr(c), s, partner).wait_send()

    def kv_plane(g):
        return (
            lambda tt: kv_block(g, tt),
            lambda c: pk_s.at[g, c], lambda c: pk_r.at[g, c],
            lambda c: pkf_s.at[g, c], lambda c: pkf_r.at[g, c],
        )

    wo_plane = (
        wo_block,
        lambda c: pw_s.at[c], lambda c: pw_r.at[c],
        lambda c: pwf_s.at[c], lambda c: pwf_r.at[c],
    )
    row_plane = (
        row_block,
        lambda c: pr_s.at[c], lambda c: pr_r.at[c],
        lambda c: prf_s.at[c], lambda c: prf_r.at[c],
    )

    for c in kv_loc:
        c.wait()
    plane_send(*kv_plane(s))
    for g in range(S):
        @pl.when(s != g)
        def _():
            d = lax.rem(s - g + S, S)
            for i in range(2):
                remote(
                    kv_part(g, i), kv_part(g, i), kvz_s.at[d - 1, i], kvz_r.at[d - 1, i], g, t
                ).wait_recv()
            plane_send(*kv_plane(g))

    def attention(g):
        first_row = g * segment_len + t * rows
        for h in range(kv_local):
            for e in range(group):
                head = h * group + e
                qt_ref[h, :, e * rows : (e + 1) * rows] = q_all[
                    g, :, head * HEAD_DIM : (head + 1) * HEAD_DIM
                ].T
        acc_ref[...] = jnp.zeros_like(acc_ref)

        def step(chunk, carry, masked):
            first = al(chunk * KEY_CHUNK, KEY_CHUNK)
            scores = []
            for h in range(kv_local):
                k = kv_all[pl.ds(first, KEY_CHUNK), h * HEAD_DIM : (h + 1) * HEAD_DIM]
                sc = jnp.dot(k, qt_ref[h], preferred_element_type=jnp.float32)
                if masked:
                    key_pos = first + lax.broadcasted_iota(jnp.int32, (KEY_CHUNK, width), 0)
                    lane = lax.broadcasted_iota(jnp.int32, (KEY_CHUNK, width), 1)
                    sc = jnp.where(key_pos <= first_row + lax.rem(lane, rows), sc, -1e30)
                scores.append(sc)
            result = []
            for h in range(kv_local):
                peak, total = carry[h]
                sc = scores[h]
                new_peak = jnp.maximum(peak, jnp.max(sc, axis=0, keepdims=True))
                p = jnp.exp2((sc - new_peak) * LOG2_SCALE)
                fade = jnp.exp2((peak - new_peak) * LOG2_SCALE)
                total = total * fade + jnp.sum(p, axis=0, keepdims=True)
                v_at = KG + h * HEAD_DIM
                v = kv_all[pl.ds(first, KEY_CHUNK), v_at : v_at + HEAD_DIM]
                acc_ref[h] = acc_ref[h] * fade + lax.dot_general(
                    v, p.astype(jnp.bfloat16), (((0,), (0,)), ((), ())),
                    preferred_element_type=jnp.float32,
                )
                result.append((new_peak, total))
            return tuple(result)

        carry = tuple(
            (jnp.full((1, width), -1e30, jnp.float32), jnp.zeros((1, width), jnp.float32))
            for _ in range(kv_local)
        )
        whole_chunks = first_row // KEY_CHUNK
        carry = lax.fori_loop(0, whole_chunks, lambda i, c: step(i, c, False), carry)
        carry = step(whole_chunks, carry, True)
        for h in range(kv_local):
            mixed = (acc_ref[h] / carry[h][1]).astype(jnp.bfloat16)
            for e in range(group):
                head = h * group + e
                attn_out[g, :, head * HEAD_DIM : (head + 1) * HEAD_DIM] = mixed[
                    :, e * rows : (e + 1) * rows
                ].T

    def attn_copy(g):
        d = lax.rem(g - s + S, S)
        return remote(
            attn_out.at[g], attn_full.at[:, pl.ds(al(s * HG, HG), HG)],
            az_s.at[d - 1], az_r.at[d - 1], g, t,
        )

    def wo_z_wait():
        wo_loc.wait()
        for d in range(1, S):
            src = lax.rem(s - d + S, S)
            remote(wo_piece(src), wo_piece(src), woz_s.at[d - 1], woz_r.at[d - 1], src, t).wait_recv()

    for d in range(1, S):
        woz(d).start()
    for m in (GATE, UP):
        w_pass(m, 0)
    plane_forward(*kv_plane(0))
    for g in range(S):
        if g + 1 < S:
            plane_forward(*kv_plane(g + 1))
        plane_corner(*kv_plane(g))
        if g == S - 1:
            wo_z_wait()
            plane_send(*wo_plane)

        @pl.when(s == g)
        def _():
            q_loc.wait()

        @pl.when(s != g)
        def _():
            d = lax.rem(s - g + S, S)
            remote(q_all.at[g], q_all.at[g], qz_s.at[d - 1], qz_r.at[d - 1], g, t).wait_recv()

        plane_wait(*kv_plane(g))
        attention(g)

        @pl.when(s == g)
        def _():
            attn_full[:, pl.ds(al(s * HG, HG), HG)] = attn_out[g]

        @pl.when(s != g)
        def _():
            attn_copy(g).start()

    plane_forward(*wo_plane)
    for m in (GATE, UP):
        if S > 2:
            w_pass(m, 1)
    plane_corner(*wo_plane)

    plane_wait(*wo_plane)
    for d in range(1, S):
        src = lax.rem(s - d + S, S)
        piece = attn_full.at[:, pl.ds(al(src * HG, HG), HG)]
        remote(piece, piece, az_s.at[d - 1], az_r.at[d - 1], src, t).wait_recv()

    tile = DG

    def project(n, squares):
        at = pl.ds(al(n * tile, tile), tile)
        total = jnp.dot(attn_full[...], wo_full[:, at], preferred_element_type=jnp.float32)
        a = (tok_ref[:, at].astype(jnp.float32) + total).astype(jnp.bfloat16)
        att_ref[:, at] = a
        wide = a.astype(jnp.float32)
        return squares + jnp.sum(wide * wide, axis=1, keepdims=True)

    squares = lax.fori_loop(0, S, project, jnp.zeros((rows, 1), jnp.float32))
    inverse_rms = lax.rsqrt(squares * (1.0 / D) + norm_eps)
    my_rows = pl.ds(al(t * rows, rows), rows)
    rows_all[my_rows, :] = (
        att_ref[...].astype(jnp.float32) * inverse_rms * gain_ref[...].reshape(1, D).astype(jnp.float32)
    ).astype(jnp.bfloat16)
    plane_send(*row_plane)

    for d in range(2, S - 1):
        w_pass(GATE, d)
        if d == 2:
            plane_forward(*row_plane)
        w_pass(UP, d)
    if S <= 3:
        plane_forward(*row_plane)
    for m in range(DOWN, DOWN + SUB):
        w_pass(m, 0)
    plane_corner(*row_plane)
    for d in range(1, S):
        w_rest(GATE, d)
    w_loc[GATE].wait()
    plane_wait(*row_plane)
    plane_drain(*wo_plane)
    for g in range(S):
        plane_drain(*kv_plane(g))

    step_rows = 2 * rows

    def hidden_step(b, _):
        at = pl.ds(al(b * step_rows, step_rows), step_rows)
        x = rows_all[at, :]
        gate = gate_sum[at, :]
        up = jnp.dot(x, up_full[...], preferred_element_type=jnp.float32)
        wo_full[at, :F] = (gate / (1.0 + jnp.exp(-gate)) * up).astype(jnp.bfloat16)
        return 0

    def gate_step(b, _):
        at = pl.ds(al(b * step_rows, step_rows), step_rows)
        gate_sum[at, :] = jnp.dot(
            rows_all[at, :], gate_full[...], preferred_element_type=jnp.float32
        )
        return 0

    lax.fori_loop(0, half, gate_step, 0)
    for d in range(1, S):
        w_rest(UP, d)
    w_loc[UP].wait()
    lax.fori_loop(0, half // 2, hidden_step, 0)
    for m in range(DOWN, DOWN + SUB):
        w_pass(m, 1)
    lax.fori_loop(half // 2, half, hidden_step, 0)

    near = jnp.minimum(s, S - 1 - s)

    def order(k):
        far = (k + 1) // 2
        swing = s - far if k % 2 else s + far
        tail = jnp.where(s == near, k, S - 1 - k)
        return jnp.where(k <= 2 * near, swing, tail)

    mine_base = S * half * rows

    def region(j, own):
        base = jnp.where(own, mine_base, 0)
        return base + j * (half * rows)

    def pair_copy(j, h):
        at = pl.ds(al(region(j, False), rows), half * rows)
        src = kv_all.at[at, pl.ds(h * SW, SW)]
        return remote(src, pair_buf.at[j, h], pair_s.at[j, h], pair_r.at[j, h], s, partner)

    def rs_copy(j, h, c):
        block = lax.rem(t // 2 + c, half)
        at = pl.ds(al(region(j, True) + block * rows, rows), rows)
        src = kv_all.at[at, pl.ds(h * SW, SW)]
        return remote(
            src, rs_buf.at[j, h, c - 1], rs_s.at[j, h, c - 1], rs_r.at[j, h, c - 1], s, tpeer(c)
        )

    def down_step(j, h):
        cols = pl.ds(al(j * DG + h * SW, SW), SW)

        def body(b, _):
            at = pl.ds(al(b * step_rows, step_rows), step_rows)
            y = jnp.dot(wo_full[at, :F], down_full[:, cols], preferred_element_type=jnp.float32)
            y = y.astype(jnp.bfloat16)
            for e in range(2):
                to = region(j, parity == e) + b * rows
                kv_all[pl.ds(al(to, rows), rows), h * SW : (h + 1) * SW] = y[
                    e * rows : (e + 1) * rows
                ]
            return 0

        lax.fori_loop(0, half, body, 0)
        pair_copy(j, h).start()

    def reduce_step(j, h):
        pair_copy(j, h).wait_recv()
        for c in range(1, half):
            block = lax.rem(t // 2 + c, half)
            at = pl.ds(al(region(j, True) + block * rows, rows), rows)
            cols = slice(h * SW, (h + 1) * SW)
            other = pair_buf[j, h, pl.ds(al(block * rows, rows), rows), :]
            kv_all[at, cols] = (
                kv_all[at, cols].astype(jnp.float32) + other.astype(jnp.float32)
            ).astype(jnp.bfloat16)
            rs_copy(j, h, c).start()

    mine = t // 2

    def finish(j, h):
        cols = pl.ds(al(j * DG + h * SW, SW), SW)
        for c in range(1, half):
            rs_copy(j, h, c).wait_recv()
        at = pl.ds(al(region(j, True) + mine * rows, rows), rows)
        total = att_ref[:, cols].astype(jnp.float32)
        total += kv_all[at, h * SW : (h + 1) * SW].astype(jnp.float32)
        total += pair_buf[j, h, pl.ds(al(mine * rows, rows), rows), :].astype(jnp.float32)
        for c in range(1, half):
            total += rs_buf[j, h, c - 1].astype(jnp.float32)
        out_ref[:, cols] = total.astype(jnp.bfloat16)

    steps = [(k, h) for k in range(S) for h in range(SUB)]
    for i, (k, h) in enumerate(steps):
        j = order(k)
        if h == 0 and 2 <= k + 1 < S - 1:
            for m in range(DOWN, DOWN + SUB):
                w_pass(m, k + 1)
        if k >= 1:
            w_rest(DOWN + h, k)
        elif h == 0:
            for m in range(DOWN, DOWN + SUB):
                w_loc[m].wait()
        down_step(j, h)
        if i >= 1:
            reduce_step(order(steps[i - 1][0]), steps[i - 1][1])
        if i >= LAG:
            finish(order(steps[i - LAG][0]), steps[i - LAG][1])
    k, h = steps[-1]
    reduce_step(order(k), h)
    for k, h in steps[max(len(steps) - LAG, 0):]:
        finish(order(k), h)

    for d in range(1, S):
        for i in range(2):
            kvz(d, i).wait_send()
        qz(d).wait_send()
        woz(d).wait_send()
    for g in range(S):
        @pl.when(s != g)
        def _():
            attn_copy(g).wait_send()
    for m in range(DOWN + SUB):
        for d in range(S - 1):
            w_sends(m, d, lambda copy: copy.wait_send())
    plane_drain(*row_plane)
    for j in range(S):
        for h in range(SUB):
            pair_copy(j, h).wait_send()
            for c in range(1, half):
                rs_copy(j, h, c).wait_send()


def shards(
    tokens, queries, keys, values, out_weight, norm_gain, gate_weight, up_weight, down_weight
):
    S = lax.axis_size("sp")
    T = lax.axis_size("tp")
    rows, D = tokens.shape
    HG = queries.shape[1] // S
    KG = keys.shape[1] // S
    DG = D // S
    F = gate_weight.shape[1]
    half = T // 2
    SUB = parts_of(DG)
    kv_local = KG // HEAD_DIM
    width = HG // KG * rows
    assert T % 2 == 0 and 2 * KG == DG and T * rows == S * HG and F <= D
    bf16, f32 = jnp.bfloat16, jnp.float32
    vmem, any_ = pl.BlockSpec(memory_space=pltpu.VMEM), pl.BlockSpec(memory_space=pl.ANY)
    sem = pltpu.SemaphoreType.DMA
    line = S - 1
    links = 4 if half == 4 else half - 1
    return pl.pallas_call(
        functools.partial(layer_kernel, S, T),
        out_shape=(
            jax.ShapeDtypeStruct((rows, D), bf16),
            jax.ShapeDtypeStruct((rows, D), bf16),
        ),
        in_specs=[vmem, vmem] + [any_] * 7,
        out_specs=(vmem, vmem),
        scratch_shapes=[
            pltpu.VMEM((S * T * rows, 2 * KG), bf16),
            pltpu.VMEM((S, rows, HG), bf16),
            pltpu.VMEM((kv_local, HEAD_DIM, width), bf16),
            pltpu.VMEM((kv_local, HEAD_DIM, width), f32),
            pltpu.VMEM((S, rows, HG), bf16),
            pltpu.VMEM((rows, S * HG), bf16),
            pltpu.VMEM((S * HG, D), bf16),
            pltpu.VMEM((T * rows, D), bf16),
            pltpu.VMEM((D, F), bf16),
            pltpu.VMEM((D, F), bf16),
            pltpu.VMEM((F, D), bf16),
            pltpu.VMEM((S, SUB, half * rows, DG // SUB), bf16),
            pltpu.VMEM((S, SUB, half - 1, rows, DG // SUB), bf16),
            pltpu.VMEM((T * rows, F), f32),
            sem((6 + SUB,)),
            sem((line, 2)), sem((line, 2)), sem((line,)), sem((line,)),
            sem((line,)), sem((line,)), sem((line,)), sem((line,)),
            sem((S, links)), sem((S, links)), sem((S, half)), sem((S, half)),
            sem((links,)), sem((links,)), sem((half,)), sem((half,)),
            sem((links,)), sem((links,)), sem((half,)), sem((half,)),
            sem((2 + SUB, line, 2)), sem((2 + SUB, line, 2)),
            sem((S, SUB)), sem((S, SUB)), sem((S, SUB, half - 1)), sem((S, SUB, half - 1)),
        ],
        compiler_params=pltpu.CompilerParams(
            collective_id=0,
            has_side_effects=True,
            vmem_limit_bytes=67_043_328,
        ),
    )(
        tokens, norm_gain, queries, keys, values, out_weight,
        gate_weight, up_weight, down_weight,
    )


def solution(mesh):
    return jax.shard_map(
        shards,
        mesh=mesh,
        in_specs=(
            P(("sp", "tp"), None),
            P(("sp", "tp"), None),
            P(("sp", "tp"), None),
            P(("sp", "tp"), None),
            P("sp", "tp"),
            P(),
            P("sp", "tp"),
            P("sp", "tp"),
            P("tp", "sp"),
        ),
        out_specs=(P(("sp", "tp"), None), P(("sp", "tp"), None)),
        check_vma=False,
    )
```
